32 devices in a mesh: gx: 2 (over core), gy: 4 (over y, x), ma: 4 (over z).
Axes of the slice: x: 2, y: 2, z: 4, core: 2. Of those that a mesh axis runs over, the one named last changes fastest.
Arguments:
- object_field: float32 [2, 256, 1024], P(None, 'gx', 'gy'), may hold values from -5 to 5
- probe_modes: float32 [8, 2, 256, 256], P('ma'), may hold values from -1.5 to 1.5
- measured: float32 [2, 4, 2, 256, 256], P('gx', 'gy'), may hold values from 0.1 to 4
- positions: int32 [2, 4, 2, 2], P('gx', 'gy'), may hold values from 0 to 255, as said below
- slot_counts: int32 [2, 4], P('gx', 'gy'), may hold values from 1 to 2, as said below
Outputs:
- updated_object: float32 [2, 256, 1024], P(None, 'gx', 'gy')
The draws below stay inside these ranges and needn't reach their ends.
Inputs may be any that keep to these rules, and one draw needn't show every extreme that they name: positions[a, b, s] holds a row 0 to 127 and a column 0 to 255 of tile (a, b); slots s >= slot_counts[a, b] are unused. `slot_counts`: some tile uses all 2 slots.
All inputs are finite; a program needn't handle non-finite values.
Results may differ from the reference program's by a relative error of at most 0.0023.
Values sent between devices are 32-bit elements; how exact they have to be, the bound alone decides.
A program may use at most 64 MiB of HBM per device.

```python
import math
import jax
import jax.numpy as jnp
from jax import lax

PATCH = 256
MODES = 8
TX = 128
TY = 256
CAP = 2
OUTER = 2
ITERS = 1
GRID_X = 2
GRID_Y = 4
NX = 256
NY = 1024


def draw_positions(key, part):
    row_draw = jax.random.randint(jax.random.fold_in(key, 11), (GRID_X, GRID_Y, CAP, 1), 0, TX, dtype=jnp.int32)
    col_draw = jax.random.randint(jax.random.fold_in(key, 12), (GRID_X, GRID_Y, CAP, 1), 0, TY, dtype=jnp.int32)
    return jnp.concatenate([row_draw, col_draw], -1).astype(jnp.int32)


def draw_slot_counts(key, part):
    base_counts = jax.random.randint(jax.random.fold_in(key, 21), (GRID_X, GRID_Y), 1, CAP + 1, dtype=jnp.int32)
    chosen = jax.random.randint(jax.random.fold_in(key, 22), (), 0, GRID_X * GRID_Y, dtype=jnp.int32)
    tile_ids = jnp.arange(GRID_X * GRID_Y, dtype=jnp.int32).reshape(GRID_X, GRID_Y)
    return jnp.where(tile_ids == chosen, CAP, base_counts).astype(jnp.int32)


def level_of(key, shape, pieces, least, top_value):
    gain, own = 1.0, jax.random.fold_in(key, 6)
    for dim, blocks in pieces:
        heights = jnp.exp(jax.random.uniform(jax.random.fold_in(own, dim), (blocks,), jnp.float32, least / len(pieces), top_value / len(pieces)))
        gain = gain * jnp.repeat(heights, shape[dim] // blocks).reshape([-1 if axis == dim else 1 for axis in range(len(shape))])
    return gain


def noise(stream_key, extent, deviation, reach, pieces=(), kind=jnp.bfloat16):
    values = jax.random.normal(stream_key, extent, jnp.float32) * deviation
    if len(pieces) > 0:
        values = level_of(stream_key, extent, pieces, -0.22, 0.18) * values
    return jnp.clip(values, min=-reach, max=reach).astype(kind)


def setup_inputs(seed: int = 0) -> dict:
    streams_of = jax.random.split(jax.random.key(seed), 6)
    object_field = noise(streams_of[0], (2, NX, NY), 0.7, 5.0, ((1, 2), (2, 4)), jnp.float32)
    probe_modes = noise(streams_of[1], (MODES, 2, PATCH, PATCH), 0.25, 1.5, ((0, 4),), jnp.float32)
    measured = jnp.clip(jnp.exp(math.log(4.0) - 3.6888794 * jax.random.uniform(streams_of[2], (GRID_X, GRID_Y, CAP, PATCH, PATCH), jnp.float32) ** level_of(streams_of[2], (GRID_X, GRID_Y, CAP, PATCH, PATCH), ((0, 2), (1, 4)), -0.2, 0.2)), 0.1, 4.0)
    positions = draw_positions(jax.random.fold_in(streams_of[5], 71), 0)
    slot_counts = draw_slot_counts(jax.random.fold_in(streams_of[5], 71), 0)
    return {"object_field": object_field, "probe_modes": probe_modes, "measured": measured, "positions": positions, "slot_counts": slot_counts}


DAMPING = 1.0

def dft_tables(patch_width):
    ladder = jnp.arange(patch_width, dtype=jnp.int32)
    phases = ladder[:, None] * ladder[None, :] % patch_width
    angles = phases.astype(jnp.float32) * (2.0 * math.pi / patch_width)
    factor = 1.0 / math.sqrt(patch_width)
    real_part = jnp.cos(angles) * factor
    imag_part = -jnp.sin(angles) * factor
    table_one = jnp.concatenate([jnp.concatenate([real_part, -imag_part], 1), jnp.concatenate([imag_part, real_part], 1)], 0).astype(jnp.bfloat16)
    table_two = jnp.concatenate([jnp.concatenate([real_part, imag_part], 1), jnp.concatenate([-imag_part, real_part], 1)], 0).astype(jnp.bfloat16)
    return (table_one, table_two)

def forward_ref(wavefield, tables):
    patch_width = wavefield.shape[-1]
    first_table = tables[0].astype(jnp.float32).reshape(2, patch_width, 2, patch_width)
    second_table = tables[1].astype(jnp.float32).reshape(2, patch_width, 2 * patch_width)
    halfway = jnp.einsum('pqci,bcik->bpqk', first_table, wavefield.astype(jnp.float32)).astype(jnp.bfloat16)
    halfway = lax.optimization_barrier(halfway)
    return jnp.einsum('bcik,ckl->bil', halfway.astype(jnp.float32), second_table)

def adjoint_ref(weighted, tables):
    patch_width = weighted.shape[1]
    halfway = jnp.einsum('bik,kl->bil', weighted.astype(jnp.float32), tables[0].astype(jnp.float32)).astype(jnp.bfloat16)
    halfway = lax.optimization_barrier(halfway)
    second_table = tables[1].astype(jnp.float32).reshape(2, patch_width, 2, patch_width)
    return jnp.einsum('pqci,bicl->bpql', second_table, halfway.astype(jnp.float32).reshape(halfway.shape[0], patch_width, 2, patch_width))

def exit_waves(probe_modes, windows):
    probe_real = probe_modes[None, :, 0]
    probe_imag = probe_modes[None, :, 1]
    window_real = windows[:, None, 0]
    window_imag = windows[:, None, 1]
    real_part = probe_real * window_real - probe_imag * window_imag
    imag_part = probe_real * window_imag + probe_imag * window_real
    wavefield = jnp.stack([real_part, imag_part], 2).astype(jnp.bfloat16)
    wavefield = lax.optimization_barrier(wavefield)
    return wavefield.reshape(-1, 2, probe_modes.shape[-1], probe_modes.shape[-1])

def intensity_part(spectra, mode_count):
    patch_width = spectra.shape[1]
    grouped = spectra.reshape(-1, mode_count, patch_width, 2 * patch_width)
    squared = grouped * grouped
    return lax.optimization_barrier(jnp.sum(squared[..., :patch_width] + squared[..., patch_width:], axis=1))

def change_part(spectra, moved_spectra, mode_count):
    patch_width = spectra.shape[1]
    grouped = spectra.reshape(-1, mode_count, patch_width, 2 * patch_width)
    shifted = moved_spectra.reshape(-1, mode_count, patch_width, 2 * patch_width)
    product = grouped * shifted
    return 2.0 * lax.optimization_barrier(jnp.sum(product[..., :patch_width] + product[..., patch_width:], axis=1))

def mode_images(weights, spectra, probe_modes, tables):
    mode_count = probe_modes.shape[0]
    patch_width = probe_modes.shape[-1]
    doubled = jnp.concatenate([weights, weights], -1)
    grouped = spectra.reshape(-1, mode_count, patch_width, 2 * patch_width)
    weighted = (2.0 * grouped * doubled[:, None]).astype(jnp.bfloat16)
    weighted = lax.optimization_barrier(weighted)
    returned = adjoint_ref(weighted.reshape(-1, patch_width, 2 * patch_width), tables)
    returned = returned.reshape(-1, mode_count, 2, patch_width, patch_width)
    probe_real = probe_modes[None, :, 0]
    probe_imag = probe_modes[None, :, 1]
    real_part = lax.optimization_barrier(jnp.sum(probe_real * returned[:, :, 0] + probe_imag * returned[:, :, 1], axis=1))
    imag_part = lax.optimization_barrier(jnp.sum(probe_real * returned[:, :, 1] - probe_imag * returned[:, :, 0], axis=1))
    return jnp.stack([real_part, imag_part], 1)

def reference(object_field, probe_modes, measured, positions, slot_counts):
    half_width = PATCH // 2
    tables = dft_tables(PATCH)
    first_rows = (jnp.arange(GRID_X, dtype=jnp.int32) * TX)[:, None, None]
    first_cols = (jnp.arange(GRID_Y, dtype=jnp.int32) * TY)[None, :, None]
    corner_rows = (positions[..., 0] + first_rows).reshape(-1).astype(jnp.int32)
    corner_cols = (positions[..., 1] + first_cols).reshape(-1).astype(jnp.int32)
    corners = jnp.stack([corner_rows, corner_cols], 1)
    live_mask = (jnp.arange(CAP, dtype=jnp.int32)[None, None, :] < slot_counts[:, :, None]).astype(jnp.float32).reshape(-1)[:, None, None]
    targets = measured.reshape(-1, PATCH, PATCH)
    anchor = jnp.zeros((), jnp.int32)

    def padded_of(current):
        return jnp.pad(current, ((0, 0), (half_width, half_width), (half_width, half_width)))

    def spectra_of(current):
        padded = padded_of(current)

        def one_pattern(corner):
            window = lax.dynamic_slice(padded, (anchor, corner[0], corner[1]), (2, PATCH, PATCH))
            return forward_ref(exit_waves(probe_modes, window[None]), tables)
        return lax.map(one_pattern, corners)

    def project(weights, spectra):
        canvas = jnp.zeros((2, NX + PATCH, NY + PATCH), jnp.float32)

        def place(canvas, inputs):
            corner, weight, spectrum = inputs
            piece = mode_images(weight[None], spectrum, probe_modes, tables)[0]
            where = (anchor, corner[0], corner[1])
            canvas = lax.dynamic_update_slice(canvas, lax.dynamic_slice(canvas, where, (2, PATCH, PATCH)) + piece, where)
            return (canvas, None)
        canvas = lax.scan(place, canvas, (corners, weights, spectra))[0]
        return canvas[:, half_width:half_width + NX, half_width:half_width + NY]
    current = object_field
    for outer_step in range(OUTER):
        spectra = spectra_of(current)

        def one_intensity(spectrum):
            return intensity_part(spectrum, MODES)[0]
        intensity = lax.map(one_intensity, spectra)
        misfit = live_mask * (intensity - targets)
        gradient = project(misfit, spectra)

        def operator(vector):
            padded = padded_of(vector)

            def one_change(inputs):
                corner, spectrum = inputs
                window = lax.dynamic_slice(padded, (anchor, corner[0], corner[1]), (2, PATCH, PATCH))
                moved_spectra = forward_ref(exit_waves(probe_modes, window[None]), tables)
                return change_part(spectrum, moved_spectra, MODES)[0]
            change = live_mask * lax.map(one_change, (corners, spectra))
            return project(change, spectra) + DAMPING * vector
        update = jnp.zeros_like(current)
        residual = -gradient
        direction = residual
        norm_now = jnp.sum(residual * residual)
        for inner_step in range(ITERS):
            applied = operator(direction)
            step_size = norm_now / jnp.sum(direction * applied)
            update = update + step_size * direction
            residual = residual - step_size * applied
            if inner_step + 1 < ITERS:
                norm_next = jnp.sum(residual * residual)
                direction = residual + norm_next / norm_now * direction
                norm_now = norm_next
        current = current + update
    return current
```

```python
import math

import jax
import jax.numpy as jnp
import numpy as np
from jax import lax
from jax.sharding import PartitionSpec as P

OUTER = 2
DAMPING = 1.0


def dft_tables(patch_width):
    ladder = np.arange(patch_width)
    angles = (ladder[:, None] * ladder[None, :] % patch_width) * (2.0 * math.pi / patch_width)
    factor = 1.0 / math.sqrt(patch_width)
    real_part = np.cos(angles) * factor
    imag_part = -np.sin(angles) * factor
    table_one = np.block([[real_part, -imag_part], [imag_part, real_part]])
    table_two = np.block([[real_part, imag_part], [-imag_part, real_part]])
    return jnp.asarray(table_one, jnp.bfloat16), jnp.asarray(table_two, jnp.bfloat16)


def shift_pair(low_part, high_part, axis):
    count = lax.axis_size(axis)
    forward = [(i, i + 1) for i in range(count - 1)]
    backward = [(target, source) for source, target in forward]
    return lax.ppermute(high_part, axis, forward), lax.ppermute(low_part, axis, backward)


def widen(block, axis, dim, width):
    size = block.shape[dim]
    low, high = shift_pair(
        lax.slice_in_dim(block, 0, width, axis=dim),
        lax.slice_in_dim(block, size - width, None, axis=dim),
        axis,
    )
    return jnp.concatenate([low, block, high], axis=dim)


def fold(block, axis, dim, width):
    size = block.shape[dim]
    low, high = shift_pair(
        lax.slice_in_dim(block, 0, width, axis=dim),
        lax.slice_in_dim(block, size - width, None, axis=dim),
        axis,
    )
    middle = lax.slice_in_dim(block, width, size - width, axis=dim)
    pads = [(0, 0)] * 3
    pads[dim] = (0, size - 3 * width)
    first = jnp.pad(low, pads)
    pads[dim] = (size - 3 * width, 0)
    return middle + first + jnp.pad(high, pads)


def shards(object_field, probe_shard, measured, positions, slot_counts):
    patch = probe_shard.shape[-1]
    rim = patch // 2
    rows, cols = object_field.shape[1:]
    slots = measured.shape[2]
    share = patch // lax.axis_size("ma")
    first = lax.axis_index("ma") * share
    table_one, table_two = dft_tables(patch)
    left_one = lax.dynamic_slice_in_dim(table_one.reshape(2, patch, 2, patch), first, share, 1)
    right_two = table_two.reshape(2, patch, 2 * patch)
    left_two = lax.dynamic_slice_in_dim(table_two.reshape(2, patch, 2, patch), first, share, 3)
    targets = lax.dynamic_slice_in_dim(measured[0, 0], first, share, 1)
    centres = positions[0, 0]
    live = (jnp.arange(slots, dtype=jnp.int32) < slot_counts[0, 0]).astype(jnp.float32)
    live = live[:, None, None]
    anchor = jnp.zeros((), jnp.int32)
    probes = lax.all_gather(probe_shard, "ma", axis=0, tiled=True)
    modes = probes.shape[0]
    probe_real, probe_imag = probes[None, :, 0], probes[None, :, 1]

    def spectra_of(tile):
        padded = widen(widen(tile, "gy", 2, rim), "gx", 1, rim)
        windows = jnp.stack(
            [
                lax.dynamic_slice(padded, (anchor, centres[s, 0], centres[s, 1]), (2, patch, patch))
                for s in range(slots)
            ]
        )
        real, imag = windows[:, None, 0], windows[:, None, 1]
        waves = jnp.stack(
            [probe_real * real - probe_imag * imag, probe_real * imag + probe_imag * real], 2
        ).astype(jnp.bfloat16)
        halfway = jnp.einsum(
            "pqci,smcik->smpqk", left_one, waves, preferred_element_type=jnp.float32
        ).astype(jnp.bfloat16)
        return jnp.einsum(
            "smcik,ckl->smil", halfway, right_two, preferred_element_type=jnp.float32
        )

    def mode_sum(first_spectra, second_spectra):
        product = first_spectra * second_spectra
        return jnp.sum(product[..., :patch] + product[..., patch:], axis=1)

    def project(weights, spectra):
        doubled = jnp.concatenate([weights, weights], -1)[:, None]
        scaled = (2.0 * spectra * doubled).astype(jnp.bfloat16)
        turned = jnp.einsum(
            "smik,kl->smil", scaled, table_one, preferred_element_type=jnp.float32
        ).astype(jnp.bfloat16)
        back = jnp.einsum(
            "pqci,smicl->smpql",
            left_two,
            turned.reshape(slots, modes, share, 2, patch),
            preferred_element_type=jnp.float32,
        )
        real = jnp.sum(probe_real * back[:, :, 0] + probe_imag * back[:, :, 1], axis=1)
        imag = jnp.sum(probe_real * back[:, :, 1] - probe_imag * back[:, :, 0], axis=1)
        pieces = jnp.stack([real, imag], 1)
        canvas = jnp.zeros((2, rows + patch, cols + patch), jnp.float32)
        room = jnp.pad(pieces, ((0, 0), (0, 0), (rows, rows), (cols, cols)))
        for s in range(slots):
            canvas = canvas + lax.dynamic_slice(
                room[s], (anchor, rows - centres[s, 0], cols - centres[s, 1]), canvas.shape
            )
        return lax.psum(fold(fold(canvas, "gx", 1, rim), "gy", 2, rim), "ma")

    current = object_field
    spectra = spectra_of(current)
    for outer_step in range(OUTER):
        misfit = live * (mode_sum(spectra, spectra) - targets)
        direction = -project(misfit, spectra)
        moved = spectra_of(direction)
        change = 2.0 * live * mode_sum(spectra, moved)
        sums = jnp.stack(
            [jnp.sum(direction * direction) / lax.axis_size("ma"), jnp.sum(change * change)]
        )
        sums = lax.psum(sums, ("gx", "gy", "ma"))
        step_size = sums[0] / (DAMPING * sums[0] + sums[1])
        current = current + step_size * direction
        if outer_step + 1 < OUTER:
            spectra = spectra + step_size * moved
    return current


def solution(mesh):
    return jax.shard_map(
        shards,
        mesh=mesh,
        in_specs=(
            P(None, "gx", "gy"),
            P("ma", None, None, None),
            P("gx", "gy", None, None, None),
            P("gx", "gy", None, None),
            P("gx", "gy"),
        ),
        out_specs=P(None, "gx", "gy"),
        check_vma=False,
    )
```

```python
import functools
import math

import jax
import jax.numpy as jnp
import numpy as np
from jax import lax
from jax.experimental import pallas as pl
from jax.experimental.pallas import tpu as pltpu
from jax.sharding import PartitionSpec as P

OUTER = 2
DAMPING = 1.0


def dft_tables(patch_width):
    ladder = np.arange(patch_width)
    angles = (ladder[:, None] * ladder[None, :] % patch_width) * (2.0 * math.pi / patch_width)
    factor = 1.0 / math.sqrt(patch_width)
    real_part = np.cos(angles) * factor
    imag_part = -np.sin(angles) * factor
    table_one = np.block([[real_part, -imag_part], [imag_part, real_part]])
    table_two = np.block([[real_part, imag_part], [-imag_part, real_part]])
    return jnp.asarray(table_one, jnp.bfloat16), jnp.asarray(table_two, jnp.bfloat16)


MESH = pl.DeviceIdType.MESH
VMEM = pl.BlockSpec(memory_space=pltpu.VMEM)


def remote(source, target, sends, recvs, slot, axis, index):
    return pltpu.make_async_remote_copy(
        src_ref=source,
        dst_ref=target,
        send_sem=sends.at[slot],
        recv_sem=recvs.at[slot],
        device_id={axis: index},
        device_id_type=MESH,
    )


def greet(lines, groups):
    barrier = pltpu.get_barrier_semaphore()

    def call(axis, index):
        pl.semaphore_signal(barrier, inc=1, device_id={axis: index}, device_id_type=MESH)

    peers = jnp.int32(0)
    for axis in lines:
        me, count = lax.axis_index(axis), lax.axis_size(axis)
        pl.when(me > 0)(functools.partial(call, axis, me - 1))
        pl.when(me < count - 1)(functools.partial(call, axis, me + 1))
        peers = peers + jnp.minimum(me, 1) + jnp.minimum(count - 1 - me, 1)
    for axis in groups:
        me, count = lax.axis_index(axis), lax.axis_size(axis)
        for step in range(1, count):
            call(axis, lax.rem(me + step, count))
        peers = peers + (count - 1)
    pl.semaphore_wait(barrier, peers)


def swap_start(axis, low_from, high_from, low_to, high_to, sends, recvs, slot):
    me, count = lax.axis_index(axis), lax.axis_size(axis)

    @pl.when(me > 0)
    def _():
        remote(low_from, high_to, sends, recvs, slot, axis, me - 1).start()

    @pl.when(me < count - 1)
    def _():
        remote(high_from, low_to, sends, recvs, slot + 1, axis, me + 1).start()


def swap_wait(axis, low_from, high_from, low_to, high_to, sends, recvs, slot):
    me, count = lax.axis_index(axis), lax.axis_size(axis)

    @pl.when(me > 0)
    def _():
        remote(low_from, high_to, sends, recvs, slot, axis, me - 1).wait_send()
        remote(high_from, low_to, sends, recvs, slot + 1, axis, me - 1).wait_recv()

    @pl.when(me == 0)
    def _():
        low_to[...] = jnp.zeros(low_to.shape, low_to.dtype)

    @pl.when(me < count - 1)
    def _():
        remote(high_from, low_to, sends, recvs, slot + 1, axis, me + 1).wait_send()
        remote(low_from, high_to, sends, recvs, slot, axis, me + 1).wait_recv()

    @pl.when(me == count - 1)
    def _():
        high_to[...] = jnp.zeros(high_to.shape, high_to.dtype)


def swap(*arguments):
    swap_start(*arguments)
    swap_wait(*arguments)


def column_halo(pad, rim, rows, cols, sends, recvs, slot):
    body = pl.ds(rim, rows)
    return (
        "gy",
        pad.at[:, body, pl.ds(rim, rim)],
        pad.at[:, body, pl.ds(cols, rim)],
        pad.at[:, body, pl.ds(0, rim)],
        pad.at[:, body, pl.ds(rim + cols, rim)],
        sends,
        recvs,
        slot,
    )


def row_halo(pad, rim, rows, cols, sends, recvs, slot):
    return (
        "gx",
        pad.at[:, pl.ds(rim, rim)],
        pad.at[:, pl.ds(rows, rim)],
        pad.at[:, pl.ds(0, rim)],
        pad.at[:, pl.ds(rim + rows, rim)],
        sends,
        recvs,
        slot,
    )


def gather_kernel(rim, probe_ref, tile_ref, probes_ref, padded_ref, all_probes, pad, sends, recvs):
    rows, cols = tile_ref.shape[1:]
    own = probe_ref.shape[0]
    half = probe_ref.shape[2] // 2
    me, count = lax.axis_index("ma"), lax.axis_size("ma")
    cell = lax.axis_index("gx")
    paired = lax.axis_size("gx") % 2 == 0
    greet(("gx", "gy"), ("ma",))
    part = lax.rem(cell, 2)
    mate = cell + 1 - 2 * part
    halves = pl.ds(pl.multiple_of(part * half, half), half) if paired else pl.ds(0, 2 * half)

    def block(owner):
        return all_probes.at[pl.ds(owner * own, own), :, halves]

    def out_copy(step):
        to = lax.rem(me + step, count)
        return remote(
            probe_ref.at[:, :, halves], block(me), sends, recvs, 3 + step, "ma", to
        )

    for step in range(1, count):
        out_copy(step).start()
    pad[:, pl.ds(rim, rows), pl.ds(rim, cols)] = tile_ref[...]
    swap(*column_halo(pad, rim, rows, cols, sends, recvs, 0))
    swap(*row_halo(pad, rim, rows, cols, sends, recvs, 2 + count + 1))
    padded_ref[...] = pad[...]
    all_probes[pl.ds(me * own, own)] = probe_ref[...]
    base = 5 + count

    def pass_on(step):
        owner = lax.rem(me + count - step, count)
        return remote(block(owner), block(owner), sends, recvs, base + step, "gx", mate)

    def arrival(step):
        owner = lax.rem(me + count - step, count)
        return remote(
            probe_ref.at[:, :, halves], block(owner), sends, recvs, 3 + step, "ma", owner
        )

    for step in range(1, count):
        arrival(step).wait_recv()
        if paired:
            pass_on(step).start()
    for step in range(1, count):
        out_copy(step).wait_send()
        if paired:
            pass_on(step).wait_send()
            pass_on(step).wait_recv()
    probes_ref[...] = all_probes[...]


def gather(probe_shard, tile):
    own, _, patch, _ = probe_shard.shape
    count = lax.axis_size("ma")
    rows, cols = tile.shape[1:]
    probes = jax.ShapeDtypeStruct((own * count, 2, patch, patch), jnp.float32)
    padded = jax.ShapeDtypeStruct((2, rows + patch, cols + patch), jnp.float32)
    return pl.pallas_call(
        functools.partial(gather_kernel, patch // 2),
        out_shape=(probes, padded),
        in_specs=[VMEM] * 2,
        out_specs=(VMEM, VMEM),
        scratch_shapes=[
            pltpu.VMEM(probes.shape, jnp.float32),
            pltpu.VMEM(padded.shape, jnp.float32),
            pltpu.SemaphoreType.DMA((5 + 2 * count,)),
            pltpu.SemaphoreType.DMA((5 + 2 * count,)),
        ],
        compiler_params=pltpu.CompilerParams(
            collective_id=0, has_side_effects=True, vmem_limit_bytes=40 << 20
        ),
    )(probe_shard, tile)


def fold_rows(tile):
    total = jnp.zeros((8, 128), jnp.float32)
    for i in range(tile.shape[0] // 8):
        for j in range(tile.shape[1] // 128):
            total = total + tile[8 * i : 8 * i + 8, 128 * j : 128 * j + 128]
    return total


def settle_kernel(
    rim, canvas_ref, padded_ref, norm_ref, gx_in, mid, gy_in, tile, ma_in, pad, sends, recvs
):
    rows, cols = tile.shape[1:]
    me, count = lax.axis_index("ma"), lax.axis_size("ma")
    share = rows // count
    greet(("gx", "gy"), ("ma",))
    swap(
        "gx",
        canvas_ref.at[:, pl.ds(0, rim)],
        canvas_ref.at[:, pl.ds(rim + rows, rim)],
        gx_in.at[0],
        gx_in.at[1],
        sends,
        recvs,
        0,
    )
    mid[...] = canvas_ref[:, rim : rim + rows]
    mid[:, :rim] += gx_in[0]
    mid[:, rows - rim :] += gx_in[1]
    swap(
        "gy",
        mid.at[:, :, pl.ds(0, rim)],
        mid.at[:, :, pl.ds(rim + cols, rim)],
        gy_in.at[0],
        gy_in.at[1],
        sends,
        recvs,
        2,
    )
    tile[...] = mid[:, :, rim : rim + cols]
    tile[:, :, :rim] += gy_in[0]
    tile[:, :, cols - rim :] += gy_in[1]

    def band(owner, start=0):
        return pl.ds(pl.multiple_of(start + owner * share, 8), share)

    def scatter(step):
        to = lax.rem(me + step, count)
        return remote(
            tile.at[:, band(to)], ma_in.at[step - 1], sends, recvs, 8 + step, "ma", to
        )

    for step in range(1, count):
        scatter(step).start()
    total = tile[:, band(me)]
    for step in range(1, count):
        scatter(step).wait_recv()
        total = total + ma_in[step - 1]
    total = -total
    pad[:, band(me, rim), pl.ds(rim, cols)] = total
    norm_ref[...] = fold_rows(total[0] * total[0] + total[1] * total[1])

    def spread(step, owner, to):
        piece = pad.at[:, band(owner, rim), pl.ds(rim, cols)]
        return remote(piece, piece, sends, recvs, 8 + count + step, "ma", to)

    for step in range(1, count):
        spread(step, me, lax.rem(me + step, count)).start()
    for step in range(1, count):
        owner = lax.rem(me + count - step, count)
        spread(step, owner, owner).wait_recv()
    swap(*column_halo(pad, rim, rows, cols, sends, recvs, 4))
    swap(*row_halo(pad, rim, rows, cols, sends, recvs, 6))
    for step in range(1, count):
        to = lax.rem(me + step, count)
        scatter(step).wait_send()
        spread(step, me, to).wait_send()
    padded_ref[...] = pad[...]


def settle(canvas, patch):
    rim = patch // 2
    rows, cols = canvas.shape[1] - patch, canvas.shape[2] - patch
    count = lax.axis_size("ma")
    f32 = jnp.float32
    return pl.pallas_call(
        functools.partial(settle_kernel, rim),
        out_shape=(
            jax.ShapeDtypeStruct(canvas.shape, f32),
            jax.ShapeDtypeStruct((8, 128), f32),
        ),
        in_specs=[VMEM],
        out_specs=(VMEM, VMEM),
        scratch_shapes=[
            pltpu.VMEM((2, 2, rim, cols + patch), f32),
            pltpu.VMEM((2, rows, cols + patch), f32),
            pltpu.VMEM((2, 2, rows, rim), f32),
            pltpu.VMEM((2, rows, cols), f32),
            pltpu.VMEM((count, 2, rows // count, cols), f32),
            pltpu.VMEM(canvas.shape, f32),
            pltpu.SemaphoreType.DMA((8 + 2 * count,)),
            pltpu.SemaphoreType.DMA((8 + 2 * count,)),
        ],
        compiler_params=pltpu.CompilerParams(
            collective_id=1, has_side_effects=True, vmem_limit_bytes=40 << 20
        ),
    )(canvas)


AXES = ("ma", "gy", "gx")


def total_kernel(value_ref, out_ref, *scratch):
    greet((), AXES)
    stages = len(AXES)
    for place, axis in enumerate(AXES):
        held, sends, recvs = scratch[place], scratch[stages + place], scratch[2 * stages + place]
        me, count = lax.axis_index(axis), lax.axis_size(axis)
        held[me] = value_ref[...] if place == 0 else value
        for step in range(1, count):
            to = lax.rem(me + step, count)
            pltpu.make_async_remote_copy(
                held.at[me], held.at[me], sends.at[step], recvs.at[step], {axis: to}, MESH
            ).start()
        for step in range(1, count):
            owner = lax.rem(me + count - step, count)
            pltpu.make_async_remote_copy(
                held.at[owner], held.at[owner], sends.at[step], recvs.at[step], {axis: owner}, MESH
            ).wait_recv()
        value = held[0]
        for index in range(1, count):
            value = value + held[index]
        for step in range(1, count):
            to = lax.rem(me + step, count)
            pltpu.make_async_remote_copy(
                held.at[me], held.at[me], sends.at[step], recvs.at[step], {axis: to}, MESH
            ).wait_send()
    out_ref[...] = value


def total(value):
    counts = [lax.axis_size(axis) for axis in AXES]
    return pl.pallas_call(
        total_kernel,
        out_shape=jax.ShapeDtypeStruct(value.shape, value.dtype),
        in_specs=[VMEM],
        out_specs=VMEM,
        scratch_shapes=[pltpu.VMEM((count, *value.shape), value.dtype) for count in counts]
        + [pltpu.SemaphoreType.DMA((count,)) for count in counts] * 2,
        compiler_params=pltpu.CompilerParams(collective_id=2, has_side_effects=True),
    )(value)


def shards(object_field, probe_shard, measured, positions, slot_counts):
    patch = probe_shard.shape[-1]
    rim = patch // 2
    rows, cols = object_field.shape[1:]
    slots = measured.shape[2]
    share = patch // lax.axis_size("ma")
    first = lax.axis_index("ma") * share
    table_one, table_two = dft_tables(patch)
    left_one = lax.dynamic_slice_in_dim(table_one.reshape(2, patch, 2, patch), first, share, 1)
    right_two = table_two.reshape(2, patch, 2 * patch)
    left_two = lax.dynamic_slice_in_dim(table_two.reshape(2, patch, 2, patch), first, share, 3)
    targets = lax.dynamic_slice_in_dim(measured[0, 0], first, share, 1)
    centres = positions[0, 0]
    live = (jnp.arange(slots, dtype=jnp.int32) < slot_counts[0, 0]).astype(jnp.float32)
    live = live[:, None, None]
    anchor = jnp.zeros((), jnp.int32)
    probes, padded_object = gather(probe_shard, object_field)
    modes = probes.shape[0]
    probe_real, probe_imag = probes[None, :, 0], probes[None, :, 1]

    def spectra_of(padded):
        windows = jnp.stack(
            [
                lax.dynamic_slice(padded, (anchor, centres[s, 0], centres[s, 1]), (2, patch, patch))
                for s in range(slots)
            ]
        )
        real, imag = windows[:, None, 0], windows[:, None, 1]
        waves = jnp.stack(
            [probe_real * real - probe_imag * imag, probe_real * imag + probe_imag * real], 2
        ).astype(jnp.bfloat16)
        halfway = jnp.einsum(
            "pqci,smcik->smpqk", left_one, waves, preferred_element_type=jnp.float32
        ).astype(jnp.bfloat16)
        return jnp.einsum(
            "smcik,ckl->smil", halfway, right_two, preferred_element_type=jnp.float32
        )

    def mode_sum(first_spectra, second_spectra):
        product = first_spectra * second_spectra
        return jnp.sum(product[..., :patch] + product[..., patch:], axis=1)

    def project(weights, spectra):
        doubled = jnp.concatenate([weights, weights], -1)[:, None]
        scaled = (2.0 * spectra * doubled).astype(jnp.bfloat16)
        turned = jnp.einsum(
            "smik,kl->smil", scaled, table_one, preferred_element_type=jnp.float32
        ).astype(jnp.bfloat16)
        back = jnp.einsum(
            "pqci,smicl->smpql",
            left_two,
            turned.reshape(slots, modes, share, 2, patch),
            preferred_element_type=jnp.float32,
        )
        real = jnp.sum(probe_real * back[:, :, 0] + probe_imag * back[:, :, 1], axis=1)
        imag = jnp.sum(probe_real * back[:, :, 1] - probe_imag * back[:, :, 0], axis=1)
        pieces = jnp.stack([real, imag], 1)
        canvas = jnp.zeros((2, rows + patch, cols + patch), jnp.float32)
        room = jnp.pad(pieces, ((0, 0), (0, 0), (rows, rows), (cols, cols)))
        for s in range(slots):
            canvas = canvas + lax.dynamic_slice(
                room[s], (anchor, rows - centres[s, 0], cols - centres[s, 1]), canvas.shape
            )
        return settle(canvas, patch)

    current = object_field
    spectra = spectra_of(padded_object)
    for outer_step in range(OUTER):
        misfit = live * (mode_sum(spectra, spectra) - targets)
        direction, norm = project(misfit, spectra)
        moved = spectra_of(direction)
        change = 2.0 * live * mode_sum(spectra, moved)
        curvature = jnp.zeros((8, 128), jnp.float32).at[0, 0].set(jnp.sum(change * change))
        sums = jnp.sum(total(jnp.stack([norm, curvature])), (1, 2))
        step_size = sums[0] / (DAMPING * sums[0] + sums[1])
        current = current + step_size * direction[:, rim : rim + rows, rim : rim + cols]
        if outer_step + 1 < OUTER:
            spectra = spectra + step_size * moved
    return current


def solution(mesh):
    return jax.shard_map(
        shards,
        mesh=mesh,
        in_specs=(
            P(None, "gx", "gy"),
            P("ma", None, None, None),
            P("gx", "gy", None, None, None),
            P("gx", "gy", None, None),
            P("gx", "gy"),
        ),
        out_specs=P(None, "gx", "gy"),
        check_vma=False,
    )
```

```python
import functools
import math

import jax
import jax.numpy as jnp
import numpy as np
from jax import lax
from jax.experimental import pallas as pl
from jax.experimental.pallas import tpu as pltpu
from jax.sharding import PartitionSpec as P

OUTER = 2
DAMPING = 1.0


def dft_tables(patch, groups):
    ladder = np.arange(patch)
    angles = (ladder[:, None] * ladder[None, :] % patch) * (2.0 * math.pi / patch)
    factor = 1.0 / math.sqrt(patch)
    real_part = np.cos(angles) * factor
    imag_part = -np.sin(angles) * factor
    one = np.block([[real_part, -imag_part], [imag_part, real_part]])
    two = np.block([[real_part, imag_part], [-imag_part, real_part]])
    share = patch // groups
    left_one = one.reshape(2, groups, share, 2 * patch).transpose(1, 0, 2, 3)
    left_two = two.reshape(2 * patch, 2, groups, share).transpose(2, 0, 1, 3)
    parts = (
        left_one.reshape(groups, 2 * share, 2 * patch),
        two,
        one,
        left_two.reshape(groups, 2 * patch, 2 * share),
    )
    return tuple(jnp.asarray(part, jnp.bfloat16) for part in parts)


MESH = pl.DeviceIdType.MESH
VMEM = pl.BlockSpec(memory_space=pltpu.VMEM)


def remote(source, target, sends, recvs, slot, axis, index):
    return pltpu.make_async_remote_copy(
        src_ref=source,
        dst_ref=target,
        send_sem=sends.at[slot],
        recv_sem=recvs.at[slot],
        device_id={axis: index},
        device_id_type=MESH,
    )


def greet(lines, groups):
    barrier = pltpu.get_barrier_semaphore()

    def call(axis, index):
        pl.semaphore_signal(barrier, inc=1, device_id={axis: index}, device_id_type=MESH)

    peers = jnp.int32(0)
    for axis in lines:
        me, count = lax.axis_index(axis), lax.axis_size(axis)
        pl.when(me > 0)(functools.partial(call, axis, me - 1))
        pl.when(me < count - 1)(functools.partial(call, axis, me + 1))
        peers = peers + jnp.minimum(me, 1) + jnp.minimum(count - 1 - me, 1)
    for axis in groups:
        me, count = lax.axis_index(axis), lax.axis_size(axis)
        for step in range(1, count):
            call(axis, lax.rem(me + step, count))
        peers = peers + (count - 1)
    pl.semaphore_wait(barrier, peers)


def swap_start(axis, low_from, high_from, low_to, high_to, sends, recvs, slot):
    me, count = lax.axis_index(axis), lax.axis_size(axis)

    @pl.when(me > 0)
    def _():
        remote(low_from, high_to, sends, recvs, slot, axis, me - 1).start()

    @pl.when(me < count - 1)
    def _():
        remote(high_from, low_to, sends, recvs, slot + 1, axis, me + 1).start()


def swap_wait(axis, low_from, high_from, low_to, high_to, sends, recvs, slot):
    me, count = lax.axis_index(axis), lax.axis_size(axis)

    @pl.when(me > 0)
    def _():
        remote(low_from, high_to, sends, recvs, slot, axis, me - 1).wait_send()
        remote(high_from, low_to, sends, recvs, slot + 1, axis, me - 1).wait_recv()

    @pl.when(me == 0)
    def _():
        low_to[...] = jnp.zeros(low_to.shape, low_to.dtype)

    @pl.when(me < count - 1)
    def _():
        remote(high_from, low_to, sends, recvs, slot + 1, axis, me + 1).wait_send()
        remote(low_from, high_to, sends, recvs, slot, axis, me + 1).wait_recv()

    @pl.when(me == count - 1)
    def _():
        high_to[...] = jnp.zeros(high_to.shape, high_to.dtype)


def swap(*arguments):
    swap_start(*arguments)
    swap_wait(*arguments)


def column_halo(pad, rim, rows, cols, sends, recvs, slot):
    body = pl.ds(rim, rows)
    return (
        "gy",
        pad.at[:, body, pl.ds(rim, rim)],
        pad.at[:, body, pl.ds(cols, rim)],
        pad.at[:, body, pl.ds(0, rim)],
        pad.at[:, body, pl.ds(rim + cols, rim)],
        sends,
        recvs,
        slot,
    )


def row_halo(pad, rim, rows, cols, sends, recvs, slot):
    return (
        "gx",
        pad.at[:, pl.ds(rim, rim)],
        pad.at[:, pl.ds(rows, rim)],
        pad.at[:, pl.ds(0, rim)],
        pad.at[:, pl.ds(rim + rows, rim)],
        sends,
        recvs,
        slot,
    )


def gather_kernel(rim, probe_ref, tile_ref, probes_ref, padded_ref, all_probes, pad, sends, recvs):
    rows, cols = tile_ref.shape[1:]
    own = probe_ref.shape[0]
    half = probe_ref.shape[2] // 2
    me, count = lax.axis_index("ma"), lax.axis_size("ma")
    cell = lax.axis_index("gx")
    paired = lax.axis_size("gx") % 2 == 0
    greet(("gx", "gy"), ("ma",))
    part = lax.rem(cell, 2)
    mate = cell + 1 - 2 * part
    halves = pl.ds(pl.multiple_of(part * half, half), half) if paired else pl.ds(0, 2 * half)

    def block(owner):
        return all_probes.at[pl.ds(owner * own, own), :, halves]

    def out_copy(step):
        to = lax.rem(me + step, count)
        return remote(
            probe_ref.at[:, :, halves], block(me), sends, recvs, 3 + step, "ma", to
        )

    for step in range(1, count):
        out_copy(step).start()
    pad[:, pl.ds(rim, rows), pl.ds(rim, cols)] = tile_ref[...]
    swap(*column_halo(pad, rim, rows, cols, sends, recvs, 0))
    swap(*row_halo(pad, rim, rows, cols, sends, recvs, 2 + count + 1))
    padded_ref[...] = pad[...]
    all_probes[pl.ds(me * own, own)] = probe_ref[...]
    base = 5 + count

    def pass_on(step):
        owner = lax.rem(me + count - step, count)
        return remote(block(owner), block(owner), sends, recvs, base + step, "gx", mate)

    def arrival(step):
        owner = lax.rem(me + count - step, count)
        return remote(
            probe_ref.at[:, :, halves], block(owner), sends, recvs, 3 + step, "ma", owner
        )

    for step in range(1, count):
        arrival(step).wait_recv()
        if paired:
            pass_on(step).start()
    for step in range(1, count):
        out_copy(step).wait_send()
        if paired:
            pass_on(step).wait_send()
            pass_on(step).wait_recv()
    probes_ref[...] = all_probes[...]


def gather(probe_shard, tile):
    own, _, patch, _ = probe_shard.shape
    count = lax.axis_size("ma")
    rows, cols = tile.shape[1:]
    probes = jax.ShapeDtypeStruct((own * count, 2, patch, patch), jnp.float32)
    padded = jax.ShapeDtypeStruct((2, rows + patch, cols + patch), jnp.float32)
    return pl.pallas_call(
        functools.partial(gather_kernel, patch // 2),
        out_shape=(probes, padded),
        in_specs=[VMEM] * 2,
        out_specs=(VMEM, VMEM),
        scratch_shapes=[
            pltpu.VMEM(probes.shape, jnp.float32),
            pltpu.VMEM(padded.shape, jnp.float32),
            pltpu.SemaphoreType.DMA((5 + 2 * count,)),
            pltpu.SemaphoreType.DMA((5 + 2 * count,)),
        ],
        compiler_params=pltpu.CompilerParams(
            collective_id=0, has_side_effects=True, vmem_limit_bytes=40 << 20
        ),
    )(probe_shard, tile)


def fold_rows(tile):
    total = jnp.zeros((8, 128), jnp.float32)
    for i in range(tile.shape[0] // 8):
        for j in range(tile.shape[1] // 128):
            total = total + tile[8 * i : 8 * i + 8, 128 * j : 128 * j + 128]
    return total


def settle_kernel(
    rim, canvas_ref, padded_ref, norm_ref, gx_in, mid, gy_in, tile, ma_in, pad, sends, recvs
):
    rows, cols = tile.shape[1:]
    me, count = lax.axis_index("ma"), lax.axis_size("ma")
    share = rows // count
    greet(("gx", "gy"), ("ma",))
    swap(
        "gx",
        canvas_ref.at[:, pl.ds(0, rim)],
        canvas_ref.at[:, pl.ds(rim + rows, rim)],
        gx_in.at[0],
        gx_in.at[1],
        sends,
        recvs,
        0,
    )
    mid[...] = canvas_ref[:, rim : rim + rows]
    mid[:, :rim] += gx_in[0]
    mid[:, rows - rim :] += gx_in[1]
    swap(
        "gy",
        mid.at[:, :, pl.ds(0, rim)],
        mid.at[:, :, pl.ds(rim + cols, rim)],
        gy_in.at[0],
        gy_in.at[1],
        sends,
        recvs,
        2,
    )
    tile[...] = mid[:, :, rim : rim + cols]
    tile[:, :, :rim] += gy_in[0]
    tile[:, :, cols - rim :] += gy_in[1]

    def band(owner, start=0):
        return pl.ds(pl.multiple_of(start + owner * share, 8), share)

    def scatter(step):
        to = lax.rem(me + step, count)
        return remote(
            tile.at[:, band(to)], ma_in.at[step - 1], sends, recvs, 8 + step, "ma", to
        )

    for step in range(1, count):
        scatter(step).start()
    total = tile[:, band(me)]
    for step in range(1, count):
        scatter(step).wait_recv()
        total = total + ma_in[step - 1]
    total = -total
    pad[:, band(me, rim), pl.ds(rim, cols)] = total
    norm_ref[...] = fold_rows(total[0] * total[0] + total[1] * total[1])

    def spread(step, owner, to):
        piece = pad.at[:, band(owner, rim), pl.ds(rim, cols)]
        return remote(piece, piece, sends, recvs, 8 + count + step, "ma", to)

    for step in range(1, count):
        spread(step, me, lax.rem(me + step, count)).start()
    for step in range(1, count):
        owner = lax.rem(me + count - step, count)
        spread(step, owner, owner).wait_recv()
    swap(*column_halo(pad, rim, rows, cols, sends, recvs, 4))
    swap(*row_halo(pad, rim, rows, cols, sends, recvs, 6))
    for step in range(1, count):
        to = lax.rem(me + step, count)
        scatter(step).wait_send()
        spread(step, me, to).wait_send()
    padded_ref[...] = pad[...]


def settle(canvas, patch):
    rim = patch // 2
    rows, cols = canvas.shape[1] - patch, canvas.shape[2] - patch
    count = lax.axis_size("ma")
    f32 = jnp.float32
    return pl.pallas_call(
        functools.partial(settle_kernel, rim),
        out_shape=(
            jax.ShapeDtypeStruct(canvas.shape, f32),
            jax.ShapeDtypeStruct((8, 128), f32),
        ),
        in_specs=[VMEM],
        out_specs=(VMEM, VMEM),
        scratch_shapes=[
            pltpu.VMEM((2, 2, rim, cols + patch), f32),
            pltpu.VMEM((2, rows, cols + patch), f32),
            pltpu.VMEM((2, 2, rows, rim), f32),
            pltpu.VMEM((2, rows, cols), f32),
            pltpu.VMEM((count, 2, rows // count, cols), f32),
            pltpu.VMEM(canvas.shape, f32),
            pltpu.SemaphoreType.DMA((8 + 2 * count,)),
            pltpu.SemaphoreType.DMA((8 + 2 * count,)),
        ],
        compiler_params=pltpu.CompilerParams(
            collective_id=1, has_side_effects=True, vmem_limit_bytes=40 << 20
        ),
    )(canvas)


AXES = ("ma", "gy", "gx")


def total_kernel(value_ref, out_ref, *scratch):
    greet((), AXES)
    stages = len(AXES)
    for place, axis in enumerate(AXES):
        held, sends, recvs = scratch[place], scratch[stages + place], scratch[2 * stages + place]
        me, count = lax.axis_index(axis), lax.axis_size(axis)
        held[me] = value_ref[...] if place == 0 else value
        for step in range(1, count):
            to = lax.rem(me + step, count)
            pltpu.make_async_remote_copy(
                held.at[me], held.at[me], sends.at[step], recvs.at[step], {axis: to}, MESH
            ).start()
        for step in range(1, count):
            owner = lax.rem(me + count - step, count)
            pltpu.make_async_remote_copy(
                held.at[owner], held.at[owner], sends.at[step], recvs.at[step], {axis: owner}, MESH
            ).wait_recv()
        value = held[0]
        for index in range(1, count):
            value = value + held[index]
        for step in range(1, count):
            to = lax.rem(me + step, count)
            pltpu.make_async_remote_copy(
                held.at[me], held.at[me], sends.at[step], recvs.at[step], {axis: to}, MESH
            ).wait_send()
    out_ref[...] = value


def total(value):
    counts = [lax.axis_size(axis) for axis in AXES]
    return pl.pallas_call(
        total_kernel,
        out_shape=jax.ShapeDtypeStruct(value.shape, value.dtype),
        in_specs=[VMEM],
        out_specs=VMEM,
        scratch_shapes=[pltpu.VMEM((count, *value.shape), value.dtype) for count in counts]
        + [pltpu.SemaphoreType.DMA((count,)) for count in counts] * 2,
        compiler_params=pltpu.CompilerParams(collective_id=2, has_side_effects=True),
    )(value)


SMEM = pl.BlockSpec(memory_space=pltpu.SMEM)


def aligned_rows(row, patch):
    base = row // 8
    return pl.ds(pl.multiple_of(base * 8, 8), patch + 8), row - base * 8


def transform_slot(slot, centres, padded_ref, probes_ref, left, right, spectra_ref, window, stack):
    modes, _, patch, _ = probes_ref.shape
    share = left.shape[0] // 2
    width = padded_ref.shape[2]
    shift = lax.rem(width - centres[slot, 1], width)
    rows, offset = aligned_rows(centres[slot, 0], patch)
    tall = patch + 8
    for part in range(2):
        band = pltpu.roll(padded_ref[part, rows, :], shift, 1)[:, :patch]
        window[part] = pltpu.roll(band, lax.rem(tall - offset, tall), 0)[:patch]

    def one_mode(mode, carry):
        probe_real, probe_imag = probes_ref[mode, 0], probes_ref[mode, 1]
        real = (probe_real * window[0] - probe_imag * window[1]).astype(jnp.bfloat16)
        imag = (probe_real * window[1] + probe_imag * window[0]).astype(jnp.bfloat16)
        half = jnp.dot(
            left, jnp.concatenate([real, imag], 0), preferred_element_type=jnp.float32
        ).astype(jnp.bfloat16)
        rows = pl.ds(pl.multiple_of(mode * share, share), share)
        stack[rows, :] = jnp.concatenate([half[:share], half[share:]], 1)
        return carry

    lax.fori_loop(0, modes, one_mode, 0, unroll=2)
    result = jnp.dot(stack[...], right, preferred_element_type=jnp.float32)
    for mode in range(modes):
        spectra_ref[slot, mode] = result[mode * share : (mode + 1) * share]


def project_slot(slot, centres, weights, spectra_ref, probes_ref, table, left, canvas, piece, stack):
    modes, _, patch, _ = probes_ref.shape
    share = weights.shape[0]
    width = canvas.shape[2]
    doubled = jnp.concatenate([weights, weights], 1)
    for mode in range(modes):
        stack[mode * share : (mode + 1) * share] = (
            2.0 * spectra_ref[slot, mode] * doubled
        ).astype(jnp.bfloat16)
    turned = jnp.dot(stack[...], table, preferred_element_type=jnp.float32)
    stack[...] = turned.astype(jnp.bfloat16)
    piece[...] = jnp.zeros(piece.shape, jnp.float32)

    def one_mode(mode, carry):
        rows = stack[pl.ds(pl.multiple_of(mode * share, share), share), :]
        back = jnp.dot(
            left,
            jnp.concatenate([rows[:, :patch], rows[:, patch:]], 0),
            preferred_element_type=jnp.float32,
        )
        real, imag = back[:patch], back[patch:]
        probe_real, probe_imag = probes_ref[mode, 0], probes_ref[mode, 1]
        piece[0] += probe_real * real + probe_imag * imag
        piece[1] += probe_real * imag - probe_imag * real
        return carry

    lax.fori_loop(0, modes, one_mode, 0, unroll=2)
    rows, offset = aligned_rows(centres[slot, 0], patch)
    low = jnp.zeros((8, patch), jnp.float32)
    blank = jnp.zeros((patch + 8, width - patch), jnp.float32)
    for part in range(2):
        moved = pltpu.roll(jnp.concatenate([piece[part], low], 0), offset, 0)
        moved = pltpu.roll(jnp.concatenate([moved, blank], 1), centres[slot, 1], 1)
        canvas[part, rows, :] += moved


def misfit_of(slot, counts, measured_ref, spectra_ref):
    modes, share, double = spectra_ref.shape[1:]
    patch = double // 2
    intensity = jnp.zeros((share, patch), jnp.float32)
    for mode in range(modes):
        spectrum = spectra_ref[slot, mode]
        square = spectrum * spectrum
        intensity = intensity + (square[:, :patch] + square[:, patch:])
    first = pl.multiple_of(lax.axis_index("ma") * share, share)
    live = jnp.where(slot < counts[0, 0], 1.0, 0.0)
    return live * (intensity - measured_ref[slot, pl.ds(first, share), :])


def first_kernel(
    centres, counts, padded_ref, probes_ref, measured_ref, left_one, right, table, left_two,
    spectra_ref, canvas, window, stack,
):
    group = lax.axis_index("ma")
    canvas[...] = jnp.zeros(canvas.shape, jnp.float32)
    for slot in range(measured_ref.shape[0]):
        transform_slot(
            slot, centres, padded_ref, probes_ref, left_one[group], right[...],
            spectra_ref, window, stack,
        )
        weights = misfit_of(slot, counts, measured_ref, spectra_ref)
        project_slot(
            slot, centres, weights, spectra_ref, probes_ref, table[...], left_two[group],
            canvas, window, stack,
        )


def later_kernel(
    centres, counts, sums_ref, old_ref, moved_ref, probes_ref, measured_ref, table, left_two,
    spectra_ref, canvas, window, stack,
):
    group = lax.axis_index("ma")
    norm = jnp.sum(sums_ref[0], keepdims=True)
    step_size = norm / (DAMPING * norm + jnp.sum(sums_ref[1], keepdims=True))
    canvas[...] = jnp.zeros(canvas.shape, jnp.float32)
    for slot in range(measured_ref.shape[0]):
        for mode in range(probes_ref.shape[0]):
            spectra_ref[slot, mode] = old_ref[slot, mode] + step_size * moved_ref[slot, mode]
        weights = misfit_of(slot, counts, measured_ref, spectra_ref)
        project_slot(
            slot, centres, weights, spectra_ref, probes_ref, table[...], left_two[group],
            canvas, window, stack,
        )


def change_kernel(
    centres, counts, padded_ref, probes_ref, spectra_ref, norm_ref, left_one, right,
    moved_ref, sums_ref, window, stack,
):
    group = lax.axis_index("ma")
    slots, modes, share, double = spectra_ref.shape
    patch = double // 2
    curvature = jnp.zeros((8, 128), jnp.float32)
    for slot in range(slots):
        transform_slot(
            slot, centres, padded_ref, probes_ref, left_one[group], right[...],
            moved_ref, window, stack,
        )
        change = jnp.zeros((share, patch), jnp.float32)
        for mode in range(modes):
            product = spectra_ref[slot, mode] * moved_ref[slot, mode]
            change = change + (product[:, :patch] + product[:, patch:])
        live = jnp.where(slot < counts[0, 0], 2.0, 0.0)
        change = live * change
        curvature = curvature + fold_rows(change * change)
    sums_ref[0] = norm_ref[...]
    sums_ref[1] = curvature


def local_call(kernel, operands, shapes, patch, share, modes):
    f32 = jnp.float32
    return pl.pallas_call(
        kernel,
        out_shape=tuple(jax.ShapeDtypeStruct(shape, f32) for shape in shapes),
        in_specs=[SMEM, SMEM] + [VMEM] * (len(operands) - 2),
        out_specs=(VMEM,) * len(shapes),
        scratch_shapes=[
            pltpu.VMEM((2, patch, patch), f32),
            pltpu.VMEM((modes * share, 2 * patch), jnp.bfloat16),
        ],
        compiler_params=pltpu.CompilerParams(vmem_limit_bytes=48 << 20),
    )(*operands)


def shards(object_field, probe_shard, measured, positions, slot_counts):
    patch = probe_shard.shape[-1]
    rim = patch // 2
    rows, cols = object_field.shape[1:]
    slots = measured.shape[2]
    groups = lax.axis_size("ma")
    share = patch // groups
    modes = probe_shard.shape[0] * groups
    left_one, right, table, left_two = dft_tables(patch, groups)
    targets, centres = measured[0, 0], positions[0, 0]
    probes, padded_object = gather(probe_shard, object_field)
    spectra_shape = (slots, modes, share, 2 * patch)
    run = functools.partial(local_call, patch=patch, share=share, modes=modes)
    current = object_field
    for outer_step in range(OUTER):
        if outer_step == 0:
            spectra, canvas = run(
                first_kernel,
                (centres, slot_counts, padded_object, probes, targets, left_one, right, table, left_two),
                (spectra_shape, padded_object.shape),
            )
        else:
            spectra, canvas = run(
                later_kernel,
                (centres, slot_counts, sums, spectra, moved, probes, targets, table, left_two),
                (spectra_shape, padded_object.shape),
            )
        direction, norm = settle(canvas, patch)
        moved, sums = run(
            change_kernel,
            (centres, slot_counts, direction, probes, spectra, norm, left_one, right),
            (spectra_shape, (2, 8, 128)),
        )
        sums = total(sums)
        norms = jnp.sum(sums, (1, 2))
        step_size = norms[0] / (DAMPING * norms[0] + norms[1])
        current = current + step_size * direction[:, rim : rim + rows, rim : rim + cols]
    return current


def solution(mesh):
    return jax.shard_map(
        shards,
        mesh=mesh,
        in_specs=(
            P(None, "gx", "gy"),
            P("ma", None, None, None),
            P("gx", "gy", None, None, None),
            P("gx", "gy", None, None),
            P("gx", "gy"),
        ),
        out_specs=P(None, "gx", "gy"),
        check_vma=False,
    )
```
